32 devices in a mesh: row: 8 (over y, x, core), col: 4 (over z).
Axes of the slice: x: 2, y: 2, z: 4, core: 2. Of those that a mesh axis runs over, the one named last changes fastest.
Arguments:
- state: float32 [2048, 4, 1024], P('row', 'col'), may hold values from -6 to 6
- coupling: bfloat16 [2048, 4, 1024], P('row', 'col'), may hold values from -2 to 2, as said below
- coupling_t: bfloat16 [2, 2048, 4, 1024], P(None, 'row', 'col'), may hold values from -2 to 2, as said below
- factor: float32 [4, 4, 256, 256], P(None, 'col', 'row'), may hold values from -0.3 to 1.3
- cofactor: float32 [4, 4, 256, 256], P(None, 'col', 'row'), may hold values from -0.3 to 1.3
- rates: float32 [4, 4, 256], P(None, 'col'), may hold values from 0.5 to 2
Outputs:
- updated_state: float32 [2048, 4, 1024], P('row', 'col')
The draws below stay inside these ranges and needn't reach their ends.
Inputs may be any that keep to these rules, and one draw needn't show every extreme that they name: coupling and coupling_t hold the same matrix A; its blocks A(i, k) are zero unless k > i. coupling_t holds the transposed blocks of the A in coupling.
All inputs are finite; a program needn't handle non-finite values.
Results may differ from the reference program's by a relative error of at most 0.0003.
Values may be sent and summed in bfloat16 or wider, within the bound.
No kernel may reach another device: no remote copies, remote signals or barrier semaphores. Data moves between devices by JAX's collectives and lax.ppermute only.
A program may use at most 64 MiB of HBM per device.

```python
import math
import jax
import jax.numpy as jnp
from jax import lax

BS = 256
STEPS = 2
NBH = 8
NB = 16
CB = 4
N_COL = 4


def coupling_blocks(seed_key, block_rows, block_cols):
    base_key = jax.random.fold_in(seed_key, 404)
    flat_rows = block_rows.reshape(-1).astype(jnp.int32)
    flat_cols = block_cols.reshape(-1).astype(jnp.int32)
    limit = 4.0 / math.sqrt(BS)

    def one_block(row_id, col_id):
        sub_key = jax.random.fold_in(base_key, row_id * NB + col_id)
        values = jax.random.normal(sub_key, (BS, BS), jnp.float32) / math.sqrt(BS)
        values = jnp.clip(values, -limit, limit)
        return jnp.where(col_id > row_id, values, 0.0)
    drawn = jax.vmap(one_block)(flat_rows, flat_cols)
    return drawn.reshape(block_rows.shape + (BS, BS))


def draw_coupling(key, part):
    col_count = NB // CB
    row_ids = jnp.arange(NBH, dtype=jnp.int32)[:, None, None]
    stored = (jnp.arange(CB, dtype=jnp.int32)[:, None] * col_count + jnp.arange(col_count, dtype=jnp.int32)[None, :])[None]
    block_rows = jnp.broadcast_to(row_ids, (NBH, CB, col_count))
    block_cols = jnp.broadcast_to(NB - 1 - stored, (NBH, CB, col_count))
    drawn = coupling_blocks(key, block_rows, block_cols)
    drawn = jnp.transpose(drawn, (0, 3, 2, 1, 4))
    return drawn.reshape(NBH * BS, col_count, CB * BS).astype(jnp.bfloat16)


def draw_coupling_t(key, part):
    col_count = NB // CB
    rotated = (jnp.arange(NBH, dtype=jnp.int32) + NBH // 2) % NBH
    stored_rows = jnp.arange(2, dtype=jnp.int32)[:, None] * NBH + rotated[None, :]
    stored_cols = jnp.arange(CB, dtype=jnp.int32)[:, None] * col_count + jnp.arange(col_count, dtype=jnp.int32)[None, :]
    block_rows = jnp.broadcast_to(stored_cols[None, None], (2, NBH, CB, col_count))
    block_cols = jnp.broadcast_to((NB - 1 - stored_rows)[:, :, None, None], (2, NBH, CB, col_count))
    drawn = coupling_blocks(key, block_rows, block_cols)
    drawn = jnp.swapaxes(drawn, -1, -2)
    drawn = jnp.transpose(drawn, (0, 1, 4, 3, 2, 5))
    return drawn.reshape(2, NBH * BS, col_count, CB * BS).astype(jnp.bfloat16)


def operator_draw(seed_key):
    col_count = NB // CB
    perturb = jax.random.normal(seed_key, (CB, col_count, BS, BS), jnp.float32)
    perturb = jnp.clip(0.3 * perturb / math.sqrt(BS), -0.3, 0.3)
    return jnp.eye(BS, dtype=jnp.float32) + perturb


def draw_factor(key, part):
    return operator_draw(jax.random.fold_in(key, 17))


def draw_cofactor(key, part):
    return operator_draw(jax.random.fold_in(key, 29))


def block_scale(own_key, dims, shards, least, largest):
    gain = 1.0
    for axis_at, blocks in shards:
        steps = jax.random.uniform(jax.random.fold_in(jax.random.fold_in(own_key, 6), axis_at), (blocks,), jnp.float32, least / len(shards), largest / len(shards))
        gain = gain * jnp.repeat(jnp.exp(steps), dims[axis_at] // blocks).reshape((-1,) + (1,) * (len(dims) - 1 - axis_at))
    return gain


def centred(stream_key, dims, scale, bound, pieces=(), held_as=jnp.bfloat16):
    entries = jax.random.normal(stream_key, dims, jnp.float32) * scale
    if len(pieces) > 0:
        entries = block_scale(stream_key, dims, pieces, -0.22, 0.18) * entries
    return jnp.clip(entries, min=-bound, max=bound).astype(held_as)


def setup_inputs(seed: int = 0) -> dict:
    key_list = jax.random.split(jax.random.key(seed), 7)
    state = centred(key_list[0], (NBH * BS, N_COL, CB * BS), 1.0, 6.0, ((0, 8), (1, 4)), jnp.float32)
    coupling = draw_coupling(jax.random.fold_in(key_list[6], 71), 0)
    coupling_t = draw_coupling_t(jax.random.fold_in(key_list[6], 71), 0)
    factor = draw_factor(jax.random.fold_in(key_list[6], 71), 0)
    cofactor = draw_cofactor(jax.random.fold_in(key_list[6], 71), 0)
    rates = jnp.clip(jnp.exp(math.log(2.0) - 1.3862944 * jax.random.uniform(key_list[5], (CB, N_COL, BS), jnp.float32) ** block_scale(key_list[5], (CB, N_COL, BS), ((1, 4),), -0.2, 0.2)), 0.5, 2.0)
    return {"state": state, "coupling": coupling, "coupling_t": coupling_t, "factor": factor, "cofactor": cofactor, "rates": rates}


HIGHEST_PRECISION = lax.Precision.HIGHEST


def to_blocks(flattened, row_total):
    col_count = flattened.shape[1]
    shaped = flattened.reshape(row_total, BS, col_count, CB, BS)
    shaped = jnp.transpose(shaped, (0, 3, 2, 1, 4))
    return shaped.reshape(row_total, CB * col_count, BS, BS)


def from_blocks(blocks):
    row_total = blocks.shape[0]
    col_count = blocks.shape[1] // CB
    shaped = blocks.reshape(row_total, CB, col_count, BS, BS)
    shaped = jnp.transpose(shaped, (0, 3, 2, 1, 4))
    return shaped.reshape(row_total * BS, col_count, CB * BS)


def solve_block(residual, left_p, left_q, left_e, right_p, right_q, right_e):
    middle = jnp.dot(left_q, residual, precision=HIGHEST_PRECISION, preferred_element_type=jnp.float32)
    middle = jnp.dot(middle, right_q.T, precision=HIGHEST_PRECISION, preferred_element_type=jnp.float32)
    middle = middle / (left_e[:, None] + right_e[None, :])
    product = jnp.dot(left_p, middle, precision=HIGHEST_PRECISION, preferred_element_type=jnp.float32)
    return -jnp.dot(product, right_p.T, precision=HIGHEST_PRECISION, preferred_element_type=jnp.float32)


def reference(state, coupling, coupling_t, factor, cofactor, rates):
    col_count = state.shape[1]
    half_rows = NBH // 2
    blocks = to_blocks(state, NBH)
    upper_blocks = to_blocks(coupling, NBH)
    lower_blocks = to_blocks(coupling_t.reshape(NB * BS, col_count, CB * BS), NB)
    all_p = factor.reshape(NB, BS, BS)
    all_q = cofactor.reshape(NB, BS, BS)
    all_e = rates.reshape(NB, BS)
    row_ids = jnp.arange(NBH, dtype=jnp.int32)
    col_ids = jnp.arange(NB, dtype=jnp.int32)
    for wave_step in range(STEPS):
        antidiag = NB - 1 - wave_step
        partner = (antidiag - row_ids).astype(jnp.int32)
        usable = row_ids <= partner
        residual = blocks[row_ids, partner]
        solution = jax.vmap(solve_block)(residual, all_p[:NBH], all_q[:NBH], all_e[:NBH], all_p[partner], all_q[partner], all_e[partner])
        solution = jnp.where(usable[:, None, None], solution, 0.0)
        blocks = blocks.at[row_ids, partner].set(jnp.where(usable[:, None, None], solution, residual))
        mirror = (antidiag - col_ids).astype(jnp.int32)
        use_row = mirror <= col_ids
        sources = jnp.clip(jnp.where(use_row, mirror, col_ids), 0, NBH - 1).astype(jnp.int32)
        chosen = solution[sources]
        partner_blocks = jnp.where(use_row[:, None, None], chosen, jnp.swapaxes(chosen, 1, 2))
        upper_pick = jnp.clip(wave_step + col_ids, 0, NB - 1).astype(jnp.int32)

        def update_row(row_args, wave_step=wave_step, antidiag=antidiag, partner_blocks=partner_blocks, upper_pick=upper_pick):
            row_id, row_blocks, row_solution = row_args
            needed = wave_step + row_id
            stored = ((needed % NBH + half_rows) % NBH + NBH * (needed // NBH)).astype(jnp.int32)
            coupled = upper_blocks[row_id][upper_pick].astype(jnp.float32)
            transposed = lower_blocks[stored].astype(jnp.float32)
            left_terms = jnp.einsum("mab,mbc->mac", coupled, partner_blocks, precision=HIGHEST_PRECISION)
            right_terms = jnp.einsum("ab,mbc->mac", row_solution, transposed, precision=HIGHEST_PRECISION)
            targets = (row_id <= col_ids) & (row_id + col_ids < antidiag)
            return row_blocks - jnp.where(targets[:, None, None], left_terms + right_terms, 0.0)

        blocks = lax.map(update_row, (row_ids, blocks, solution))
    return from_blocks(blocks)
```

```python
import functools

import jax
import jax.numpy as jnp
from jax import lax
from jax.experimental import pallas as pl
from jax.experimental.pallas import tpu as pltpu
from jax.sharding import PartitionSpec as P


AXES = ("row", "col")
F32 = jnp.float32
BF16 = jnp.bfloat16
ROWS_BY_COLS = (((1,), (0,)), ((), ()))
ROWS_BY_ROWS = (((1,), (1,)), ((), ()))


def split(x):
    high = x.astype(BF16)
    return high, (x - high.astype(F32)).astype(BF16)


def dot(a, b, dims):
    return lax.dot_general(a, b, dims, preferred_element_type=F32)


def dot_full(a, b, dims):
    a_high, a_low = split(a)
    b_high, b_low = split(b)
    return dot(a_high, b_low, dims) + dot(a_low, b_high, dims) + dot(a_high, b_high, dims)


def dot_left_exact(a, b, dims):
    b_high, b_low = split(b)
    return dot(a, b_low, dims) + dot(a, b_high, dims)


def dot_right_exact(a, b, dims):
    a_high, a_low = split(a)
    return dot(a_low, b, dims) + dot(a_high, b, dims)


class Plan:
    def __init__(self, rows, cols):
        self.rows, self.cols = rows, cols
        self.order = 2 * rows
        self.slots = self.order // cols
        self.steps = range(0, rows, 2)

    def flat(self, row, col):
        return row * self.cols + col % self.cols

    def first_at(self, row):
        return (self.order - 1 - row) % self.cols

    def second_at(self, row):
        return (self.order - 2 - row) % self.cols

    def own(self, step):
        pairs = []
        for row in range(self.rows):
            for col in (self.first_at(row), self.second_at(row)):
                pairs.append((self.flat(row ^ step, col), self.flat(row, col)))
        return pairs

    def cross(self, step):
        pairs = []
        for row in range(self.rows):
            home = row % self.cols
            pairs.append((self.flat(row ^ step, home), self.flat(row, self.first_at(row))))
            pairs.append((self.flat(row ^ step ^ 2, home), self.flat(row, self.second_at(row))))
        return pairs

    def along_row(self, wave, distance):
        at = self.first_at if wave == 0 else self.second_at
        return [
            (self.flat(row, at(row)), self.flat(row, at(row) - distance))
            for row in range(self.rows)
        ]

    def next_row(self):
        return [
            (self.flat(row + 1, self.first_at(row + 1)), self.flat(row, self.second_at(row)))
            for row in range(self.rows - 1)
        ]

    def siblings(self):
        return [
            (self.flat(row ^ 1, col), self.flat(row, col))
            for row in range(self.rows)
            for col in range(self.cols)
        ]

    def is_source(self, row, col, wave):
        return row % self.cols == col or (self.order - 1 - wave - row) % self.cols == col

    def in_plane(self, wave, step):
        pairs = []
        for row in range(self.rows):
            for col in range(self.cols):
                there = row ^ step
                if self.is_source(there, col, wave) or self.is_source(there ^ 1, col, wave):
                    pairs.append((self.flat(there, col), self.flat(row, col)))
        return pairs


def here():
    return lax.axis_index("row"), lax.axis_index("col")


def vmem(count):
    return [pl.BlockSpec(memory_space=pltpu.VMEM)] * count


def call(body, outs, args, scratch=(), flops=0):
    return pl.pallas_call(
        body,
        out_shape=outs,
        in_specs=vmem(len(args)),
        out_specs=jax.tree.map(lambda _: pl.BlockSpec(memory_space=pltpu.VMEM), outs),
        scratch_shapes=scratch,
        cost_estimate=pl.CostEstimate(flops=flops, bytes_accessed=2**20, transcendentals=0),
    )(*args)


def at(start, size, unit):
    return pl.ds(pl.multiple_of(start, unit), size)


def pack_body(plan, slice_rows, *refs):
    p_ref, q_ref, p_sib, q_sib, e_ref = refs[:5]
    outs = refs[5:]
    count = len(plan.steps)
    row, col = here()
    mine = (row % 2) * slice_rows
    theirs = slice_rows - mine

    def fill(out, slot):
        out[at(mine, slice_rows, 8)] = p_ref[slot]
        out[at(theirs, slice_rows, 8)] = p_sib[slot]
        out[at(2 * slice_rows + mine, slice_rows, 8)] = q_ref[slot]
        out[at(2 * slice_rows + theirs, slice_rows, 8)] = q_sib[slot]

    for n, step in enumerate(plan.steps):
        there = row ^ step
        last = plan.order - 1 - there
        right = jnp.where(last % plan.cols == col, last, last - 1)
        fill(outs[n], right // plan.cols)
        left = jnp.where(there % plan.cols == col, there, there ^ 2)
        fill(outs[count + n], left // plan.cols)
        outs[count + n][pl.ds(4 * slice_rows, 8)] = jnp.broadcast_to(
            e_ref[left // plan.cols], (8, p_ref.shape[2])
        )


def gather_body(plan, size, wave, own, cross, rate_ref, ops, rates):
    row, _ = here()
    pair_rows = 2 * (size // plan.rows)
    for n, step in enumerate(plan.steps):
        own_at = ((row ^ step) // 2) * pair_rows
        cross_at = ((row ^ step ^ (2 * wave)) // 2) * pair_rows
        for part in range(2):
            piece = pl.ds(part * pair_rows, pair_rows)
            ops[part, at(cross_at, pair_rows, 8)] = cross[n][piece]
            ops[2 + part, at(own_at, pair_rows, 8)] = own[n][piece]
    rates[pl.ds(0, 1)] = cross[0][pl.ds(2 * pair_rows, 1)]
    rates[pl.ds(1, 1)] = rate_ref[(plan.order - 1 - wave - row) // plan.cols]


def solve(residual, ops, rates):
    size = residual.shape[0]
    left = jnp.broadcast_to(rates[pl.ds(0, 1)], (size, size)).T
    middle = dot_full(ops[1], residual, ROWS_BY_COLS)
    middle = dot_full(middle, ops[3], ROWS_BY_ROWS)
    middle = middle / (left + rates[pl.ds(1, 1)])
    middle = dot_full(ops[0], middle, ROWS_BY_COLS)
    return -dot_full(middle, ops[2], ROWS_BY_ROWS)


def columns(ref, slot, size):
    return ref[:, at(slot * size, size, 128)]


def first_body(plan, size, *refs):
    count = len(plan.steps)
    own, cross = refs[:count], refs[count : 2 * count]
    state_ref, rate_ref, out, ops, rates = refs[2 * count :]
    row, col = here()
    last = plan.order - 1 - row

    @pl.when(col == last % plan.cols)
    def _():
        gather_body(plan, size, 0, own, cross, rate_ref, ops, rates)
        out[...] = solve(columns(state_ref, last // plan.cols, size), ops, rates)


def second_body(plan, size, *refs):
    count = len(plan.steps)
    own, cross = refs[:count], refs[count : 2 * count]
    state_ref, upper_ref, lower_ref, rate_ref, same_ref, next_ref, out, ops, rates, held = refs[
        2 * count :
    ]
    row, col = here()
    last = plan.order - 2 - row

    @pl.when(col == last % plan.cols)
    def _():
        gather_body(plan, size, 1, own, cross, rate_ref, ops, rates)
        slot = last // plan.cols
        same = same_ref[...]
        held[...] = next_ref[...]

        @pl.when(row == plan.rows - 1)
        def _():
            held[...] = same.T

        residual = columns(state_ref, slot, size)
        residual -= dot_left_exact(columns(upper_ref, slot, size), held[...], ROWS_BY_COLS)
        residual -= dot_right_exact(same, columns(lower_ref, slot, size), ROWS_BY_COLS)
        out[...] = solve(residual, ops, rates)


def update_body(plan, size, wave, *refs):
    count = len(plan.steps)
    pieces = refs[:count]
    state_ref, upper_ref, lower_ref, shared_ref, out, held = refs[count:]
    row, col = here()
    limit = plan.order - 1 - wave
    shared = shared_ref[...]
    shared_high, shared_low = split(shared)
    for slot in range(plan.slots):
        m = col + plan.cols * slot
        view = pl.ds(slot * size, size)
        mirrored = limit - m <= m
        source = jnp.where(mirrored, limit - m, m)
        hit = (row <= m) & (row + m < limit)
        place = (source ^ row) // 2
        shift = (col + wave) // plan.cols if wave else 0
        out[:, view] = state_ref[:, view]

        @pl.when(hit)
        def _():
            for n in range(count):

                @pl.when(place == n)
                def _():
                    held[...] = pieces[n][...]

            @pl.when(jnp.logical_not(mirrored))
            def _():
                held[...] = held[...].T

            upper_slot = jnp.minimum(slot + shift, plan.slots - 1)
            upper = columns(upper_ref, upper_slot, size)
            lower = lower_ref[:, view]
            high, low = split(held[...])
            total = dot(upper, low, ROWS_BY_COLS) + dot(shared_low, lower, ROWS_BY_COLS)
            total += dot(upper, high, ROWS_BY_COLS) + dot(shared_high, lower, ROWS_BY_COLS)
            out[:, view] = state_ref[:, view] - total

        @pl.when(m == limit - row)
        def _():
            out[:, view] = shared


def on_device(state, coupling, coupling_t, factor, cofactor, rates):
    plan = Plan(lax.axis_size("row"), lax.axis_size("col"))
    rows, cols, slots = plan.rows, plan.cols, plan.slots
    size = state.shape[0]
    width = slots * size
    slice_rows = size // rows
    count = len(plan.steps)
    row, col = here()
    state = state.reshape(size, width)
    upper_first = coupling.reshape(size, width)
    lower = coupling_t.reshape(2, size, width)
    p = factor.reshape(slots, slice_rows, size)
    q = cofactor.reshape(slots, slice_rows, size)
    rates = rates.reshape(slots, 1, size)

    def shift(x, axis, distance, length):
        return lax.ppermute(x, axis, [((i - distance) % length, i) for i in range(length)])

    send = functools.partial(lax.ppermute, axis_name=AXES)
    siblings = plan.siblings()
    p_sib, q_sib = send(p, perm=siblings), send(q, perm=siblings)

    own_shape = jax.ShapeDtypeStruct((4 * slice_rows, size), F32)
    cross_shape = jax.ShapeDtypeStruct((4 * slice_rows + 8, size), F32)
    packed = call(
        functools.partial(pack_body, plan, slice_rows),
        [own_shape] * count + [cross_shape] * count,
        (p, q, p_sib, q_sib, rates),
    )
    own = [packed[0]] + [send(packed[n], perm=plan.own(plan.steps[n])) for n in range(1, count)]
    cross = [send(packed[count + n], perm=plan.cross(plan.steps[n])) for n in range(count)]

    half = rows // 2
    lower_first = shift(lower[0], "row", half, rows)
    lower_second = shift(lower[0], "row", half - 1, rows)
    upper_second = shift(upper_first, "col", cols - 1, cols)

    block = jax.ShapeDtypeStruct((size, size), F32)
    whole = jax.ShapeDtypeStruct((size, width), F32)
    ops = [pltpu.VMEM((4, size, size), F32), pltpu.VMEM((8, size), F32)]
    held = [pltpu.VMEM((size, size), F32)]
    cube = 2 * size**3

    x_first = call(
        functools.partial(first_body, plan, size), block, (*own, *cross, state, rates), ops, 12 * cube
    )
    at_next = send(x_first, perm=plan.next_row())
    first_along = [send(x_first, perm=plan.along_row(0, k)) for k in range(1, cols)]
    x_second = call(
        functools.partial(second_body, plan, size),
        block,
        (*own, *cross, state, upper_first, lower_first, rates, first_along[0], at_next),
        ops + held,
        16 * cube,
    )
    second_along = [send(x_second, perm=plan.along_row(1, k)) for k in range(1, cols)]

    def share(wave, solved, along):
        distance = (plan.order - 1 - wave - row - col) % cols
        shared = solved
        for k in range(1, cols):
            shared = jnp.where(distance == k, along[k - 1], shared)
        sibling = send(shared, perm=siblings)
        mine = (row % cols == col) | ((plan.order - 1 - wave - row) % cols == col)
        offered = jnp.where(mine, shared, sibling)
        pieces = [offered] + [
            send(offered, perm=plan.in_plane(wave, step)) for step in plan.steps[1:]
        ]
        return shared, pieces

    def update(wave, current, upper_now, lower_now, shared, pieces):
        return call(
            functools.partial(update_body, plan, size, wave),
            whole,
            (*pieces, current, upper_now, lower_now, shared),
            held,
            16 * slots * cube // 4,
        )

    shared, pieces = share(0, x_first, first_along)
    state = update(0, state, upper_first, lower_first, shared, pieces)
    shared, pieces = share(1, x_second, second_along)
    state = update(1, state, upper_second, lower_second, shared, pieces)
    return state.reshape(size, 1, width)


def solution(mesh):
    return jax.shard_map(
        on_device,
        mesh=mesh,
        in_specs=(
            P("row", "col", None),
            P("row", "col", None),
            P(None, "row", "col", None),
            P(None, "col", "row", None),
            P(None, "col", "row", None),
            P(None, "col", None),
        ),
        out_specs=P("row", "col", None),
        check_vma=False,
    )
```
